32 devices in a mesh: kpt: 2 (over x), grid: 16 (over z, y, core).
Axes of the slice: x: 2, y: 2, z: 4, core: 2. Of those that a mesh axis runs over, the one named last changes fastest.
Arguments:
- orbitals: bfloat16 [4, 2, 2, 512, 256, 256], P('kpt', None, None, 'grid'), may hold values from -6 to 6
- kweights: int32 [4], P('kpt'), may hold values from 1 to 16
- occupations: int32 [4, 2], P('kpt'), may hold values from 0 to 2
- z_basis: float32 [512, 512], replicated, may hold values from -0.25 to 0.25
- z_eigen: float32 [512], replicated, may hold values from 0.25 to 4
Outputs:
- potential: float32 [512, 256, 256], P('grid')
The draws below stay inside these ranges and needn't reach their ends.
All inputs are finite; a program needn't handle non-finite values.
Results may differ from the reference program's by a relative error of at most 0.0003.
Values sent between devices are 32-bit elements; how exact they have to be, the bound alone decides.
A program may use at most 128 MiB of HBM per device.

```python
import math
import jax
import jax.numpy as jnp
from jax import lax

NX = 256
NY = 256
NZ = 512
KPD = 2
BANDS = 2
KPOINTS = 4


def draw_kweights(key, part):
    first, second = jax.random.split(jax.random.fold_in(key, 11))
    base = jax.random.randint(first, (KPOINTS,), 1, 17)
    chosen = jax.random.randint(second, (), 0, KPOINTS)
    places = jnp.arange(KPOINTS, dtype=jnp.int32)
    return jnp.where(places == chosen, 16, base).astype(jnp.int32)


def draw_occupations(key, part):
    first, second = jax.random.split(jax.random.fold_in(key, 23))
    base = jax.random.randint(first, (KPOINTS * BANDS,), 0, 3)
    order = jax.random.permutation(second, KPOINTS * BANDS)
    mixed = jnp.where(order == 0, 0, jnp.where(order == 1, 2, base))
    return mixed.reshape(KPOINTS, BANDS).astype(jnp.int32)


def block_scale(own_key, extent, shards, low, top_value):
    def one(position, blocks):
        steps = jax.random.uniform(jax.random.fold_in(jax.random.fold_in(own_key, 6), position), (blocks,), jnp.float32, low / len(shards), top_value / len(shards))
        return jnp.repeat(jnp.exp(steps), extent[position] // blocks).reshape((-1,) + (1,) * (len(extent) - position - 1))

    loudness = one(*shards[0])
    for cut in shards[1:]:
        loudness = loudness * one(*cut)
    return loudness


def scatter_about(own_key, extent, scale, most, cuts=(), held_as=jnp.bfloat16):
    level = block_scale(own_key, extent, cuts, -0.22, 0.18) if cuts else 1.0
    values = jax.random.normal(own_key, extent, jnp.float32) * scale * level
    return jnp.minimum(jnp.maximum(values, -most), most).astype(held_as)


def setup_inputs(seed: int = 0) -> dict:
    keys = jax.random.split(jax.random.key(seed), 6)
    orbitals = scatter_about(keys[0], (KPOINTS, BANDS, 2, NZ, NX, NY), 1.0, 6.0, ((0, 2), (3, 16)))
    kweights = draw_kweights(jax.random.fold_in(keys[5], 71), 0)
    occupations = draw_occupations(jax.random.fold_in(keys[5], 71), 0)
    z_basis = scatter_about(keys[3], (NZ, NZ), NZ ** -0.5, 0.25, (), jnp.float32)
    z_eigen = jnp.clip(jnp.exp(jax.random.uniform(keys[4], (NZ,), jnp.float32, math.log(0.25), math.log(4.0))), 0.25, 4.0)
    return {"orbitals": orbitals, "kweights": kweights, "occupations": occupations, "z_basis": z_basis, "z_eigen": z_eigen}


precise = lax.Precision.HIGHEST


def reference(orbitals, kweights, occupations, z_basis, z_eigen):
    factor = (kweights[:, None] * occupations).astype(jnp.float32) / (16.0 * KPD * BANDS)

    def add_point(kpoint, running):
        values = lax.dynamic_index_in_dim(orbitals, kpoint, 0, keepdims=False).astype(jnp.float32)
        weights = lax.dynamic_index_in_dim(factor, kpoint, 0, keepdims=False)
        return running + jnp.sum(weights[:, None, None, None, None] * values * values, axis=(0, 1))

    density = lax.fori_loop(0, KPOINTS, add_point, jnp.zeros((NZ, NX, NY), jnp.float32))
    spectrum = jnp.fft.fft2(density, axes=(1, 2))
    stacked = jnp.stack([jnp.real(spectrum), jnp.imag(spectrum)]).astype(jnp.float32)
    wave_x = jnp.arange(NX).astype(jnp.float32)
    wave_y = jnp.arange(NY).astype(jnp.float32)
    shift_x = 2.0 * jnp.sin(jnp.pi * wave_x / NX)
    shift_y = 2.0 * jnp.sin(jnp.pi * wave_y / NY)
    shifted = shift_x[:, None] ** 2 + shift_y[None, :] ** 2
    factors = 1.0 / (z_eigen[:, None, None] + shifted[None])
    projected = jnp.einsum('zj,czab->cjab', z_basis, stacked, precision=precise)
    filtered = jnp.einsum('zj,cjab->czab', z_basis, projected * factors[None], precision=precise)
    potential = jnp.fft.ifft2(lax.complex(filtered[0], filtered[1]), axes=(1, 2))
    return jnp.real(potential).astype(jnp.float32)
```

```python
import jax
import jax.numpy as jnp
import numpy as np
from jax import lax
from jax.experimental import pallas as pl
from jax.experimental.pallas import tpu as pltpu
from jax.sharding import PartitionSpec as P


precise = lax.Precision.HIGH
CHUNKS = 4

MESH = pl.DeviceIdType.MESH
LANES = 128
TILE = 8
STEP = 2
AHEAD = 6
SLOTS = 3
SLACK = 4
bf16 = jnp.bfloat16
f32 = jnp.float32


def basis_tables(length):
    position = np.arange(length)
    angles = (position[:, None] * position[None, :] % length) * (2.0 * np.pi / length)
    table = np.where(position[:, None] <= length // 2, np.cos(angles), np.sin(angles))
    edges = (position == 0) | (position == length // 2)
    scaled = table * (np.where(edges, 1.0, 2.0) / length)[:, None]
    return table, scaled


def halves(table):
    high = table.astype(bf16)
    low = (table - high.astype(np.float64)).astype(bf16)
    return high, low


def split(value):
    high = value.astype(bf16)
    return high, (value - high.astype(f32)).astype(bf16)


def dot(left, right):
    return jnp.dot(left, right, preferred_element_type=f32)


def fused_kernel(
    orbitals, kweights, occupations, basis, eigen, forward_y, forward_x, inverse_x, wave_y, wave_x,
    half_out,
    block, rows, table_y, table_x, table_w, basis_rows, eigen_row, own, leaving, joined, leaped, column, projected,
    scaled_high, scaled_low, basis_high, basis_low, basis_turned, eigen_column, modes, half,
    load_sem, table_sem, x_send, x_recv, f_send, f_recv, b_send, b_recv, h_send, h_recv, h_keep,
):
    points, bands, parts, planes, nx, ny = orbitals.shape
    blocks = lax.axis_size("grid")
    step = leaving.shape[1]
    chunks = planes // step
    groups = planes // TILE
    ratio = TILE // step
    kxc = nx // blocks
    depth = blocks * TILE
    pairs = kxc // 2
    nz = basis.shape[0] * basis.shape[1]
    side = lax.axis_index("kpt")
    other = 1 - side
    me = lax.axis_index("grid")

    barrier = pltpu.get_barrier_semaphore()
    pl.semaphore_signal(barrier, inc=1, device_id={"kpt": other}, device_id_type=MESH)

    @pl.loop(1, blocks)
    def _(i):
        pl.semaphore_signal(barrier, inc=1, device_id={"grid": lax.rem(me + i, blocks)}, device_id_type=MESH)

    def load(c):
        slot = lax.rem(c, SLOTS)
        return pltpu.make_async_copy(
            orbitals.at[:, :, :, pl.ds(c * step, step)], block.at[slot], load_sem.at[slot]
        )

    for c in range(SLOTS):
        load(c).start()
    tables = [
        pltpu.make_async_copy(forward_y.at[other], table_y.at[:, pl.ds(0, LANES)], table_sem.at[0]),
        pltpu.make_async_copy(forward_y.at[side], table_y.at[:, pl.ds(LANES, LANES)], table_sem.at[1]),
        pltpu.make_async_copy(forward_x, table_x, table_sem.at[2]),
        pltpu.make_async_copy(inverse_x, table_w, table_sem.at[3]),
        pltpu.make_async_copy(basis, basis_rows, table_sem.at[4]),
        pltpu.make_async_copy(eigen, eigen_row, table_sem.at[5]),
    ]
    for copy in tables:
        copy.start()

    def send_x(c):
        return pltpu.make_async_remote_copy(
            src_ref=leaving.at[c], dst_ref=joined.at[c], send_sem=x_send.at[c], recv_sem=x_recv.at[c],
            device_id={"kpt": other}, device_id_type=MESH,
        )

    def density(c):
        slot = lax.rem(c, SLOTS)
        load(c).wait()
        strip = 32
        factors = [
            [(kweights[k] * occupations[k, b]).astype(f32) / (16.0 * points * bands) for b in range(bands)]
            for k in range(points)
        ]

        @pl.loop(0, step)
        def _(p):
            @pl.loop(0, nx // strip)
            def _(r):
                where = pl.ds(pl.multiple_of(r * strip, strip), strip)
                total = None
                for k in range(points):
                    for b in range(bands):
                        square = None
                        for part in range(parts):
                            value = block[slot, k, b, part, p, where, :].astype(f32)
                            square = value * value if square is None else square + value * value
                        term = factors[k][b] * square
                        total = term if total is None else total + term
                high, low = split(total)
                rows[where, pl.ds(0, ny)] = high
                rows[where, pl.ds(ny, ny)] = low

            line = dot(rows[...], table_y[pl.ds(0, 2 * ny), :]) + dot(
                rows[:, pl.ds(0, ny)], table_y[pl.ds(2 * ny, ny), :]
            )
            leaving[c, p] = line[:, :LANES]
            own[c, p] = line[:, LANES:]

        @pl.when(c + SLOTS < chunks)
        def _():
            load(c + SLOTS).start()

        send_x(c).start()

    def part_of(c, d):
        return pl.ds(pl.multiple_of((c * blocks + d) * (step * kxc), TILE), step * kxc)

    def place_of(c, d):
        first = ((c // ratio) * blocks + d) * TILE + lax.rem(c, ratio) * step
        return pl.ds(pl.multiple_of(first * kxc, TILE), step * kxc)

    def send_f(c, i):
        to = lax.rem(me + i, blocks)
        return pltpu.make_async_remote_copy(
            src_ref=leaped.at[part_of(c, to)], dst_ref=column.at[place_of(c, me)],
            send_sem=f_send.at[c], recv_sem=f_recv.at[c],
            device_id={"grid": to}, device_id_type=MESH,
        )

    def arrivals(sem):
        whole = column.at[pl.ds(0, (blocks - 1) * step * kxc)]
        return pltpu.make_async_copy(whole, whole, sem)

    def spectrum(c):
        send_x(c).wait_recv()

        @pl.loop(0, step // 2)
        def _(q):
            p = q * 2
            both = jnp.concatenate([own[c, p] + joined[c, p], own[c, p + 1] + joined[c, p + 1]], axis=1)
            high, low = split(both)
            result = dot(table_x[...], jnp.concatenate([high, high, low], axis=0))
            for s in range(2):
                for d in range(blocks):
                    first = ((c * blocks + d) * step + p + s) * kxc
                    leaped[pl.ds(pl.multiple_of(first, TILE), kxc), :] = result[
                        d * kxc : (d + 1) * kxc, s * LANES : (s + 1) * LANES
                    ]

        column[place_of(c, me), :] = leaped[part_of(c, me), :]

        @pl.loop(1, blocks)
        def _(i):
            send_f(c, i).start()

    def prepare():
        for copy in tables[4:]:
            copy.wait()

        @pl.loop(0, groups)
        def _(g):
            taken = basis_rows[:, pl.ds(pl.multiple_of(g * TILE, TILE), TILE), :].reshape(depth, nz)
            high, low = split(taken)
            basis_high[g] = high
            basis_low[g] = low
            high, low = split(taken.T)
            basis_turned[g, :, pl.ds(0, depth)] = high
            basis_turned[g, :, pl.ds(depth, depth)] = high
            basis_turned[g, :, pl.ds(2 * depth, depth)] = low

        eigen_column[...] = jnp.broadcast_to(eigen_row[...], (LANES, nz)).T

    def term(g, q):
        start = g * (depth * kxc) + 2 * q
        both = jnp.concatenate(
            [column[pl.ds(start, depth, stride=kxc), :], column[pl.ds(start + 1, depth, stride=kxc), :]], axis=1
        )
        high, low = split(both)
        return dot(basis_turned[g], jnp.concatenate([high, low, high], axis=0))

    def wait_f(g):
        for r in range(ratio):
            arrivals(f_recv.at[g * ratio + r]).wait()

    def gather(g):
        wait_f(g)

        @pl.loop(0, pairs)
        def _(q):
            @pl.when(g == 0)
            def _():
                projected[q] = term(g, q)

            @pl.when(g > 0)
            def _():
                projected[q] += term(g, q)

    def gather_last():
        g = groups - 1
        wait_f(g)
        across = wave_y[pl.ds(side, 1), :]

        @pl.loop(0, pairs)
        def _(q):
            total = term(g, q)
            if groups > 1:
                total = total + projected[q]
            for s in range(2):
                along = wave_x[me * kxc + 2 * q + s]
                value = total[:, s * LANES : (s + 1) * LANES] / (eigen_column[...] + (along + across))
                high, low = split(value)
                scaled_high[q, :, pl.ds(s * LANES, LANES)] = high
                scaled_low[q, :, pl.ds(s * LANES, LANES)] = low

    def send_b(c, i):
        to = lax.rem(me + i, blocks)
        return pltpu.make_async_remote_copy(
            src_ref=column.at[place_of(c, to)], dst_ref=modes.at[part_of(c, me)],
            send_sem=b_send.at[c], recv_sem=b_recv.at[c],
            device_id={"grid": to}, device_id_type=MESH,
        )

    def filtered(g):
        @pl.loop(0, pairs)
        def _(q):
            result = (
                dot(basis_high[g], scaled_high[q])
                + dot(basis_high[g], scaled_low[q])
                + dot(basis_low[g], scaled_high[q])
            )
            start = g * (depth * kxc) + 2 * q
            column[pl.ds(start, depth, stride=kxc), :] = result[:, :LANES]
            column[pl.ds(start + 1, depth, stride=kxc), :] = result[:, LANES:]

        for r in range(ratio):
            @pl.loop(1, blocks)
            def _(i):
                send_b(g * ratio + r, i).start()

        for r in range(ratio):
            modes[part_of(g * ratio + r, me), :] = column[place_of(g * ratio + r, me), :]

    def send_h(c):
        return pltpu.make_async_remote_copy(
            src_ref=half.at[c], dst_ref=half_out.at[side, pl.ds(c * step, step)],
            send_sem=h_send.at[c], recv_sem=h_recv.at[c],
            device_id={"kpt": other}, device_id_type=MESH,
        )

    def keep_h(c):
        return pltpu.make_async_copy(half.at[c], half_out.at[side, pl.ds(c * step, step)], h_keep.at[c])

    def inverse(c):
        arrivals(b_recv.at[c]).wait()

        @pl.loop(0, step // 2)
        def _(q):
            p = q * 2
            both = jnp.concatenate(
                [
                    jnp.concatenate(
                        [
                            modes[pl.ds(pl.multiple_of(((c * blocks + d) * step + p + s) * kxc, TILE), kxc), :]
                            for d in range(blocks)
                        ],
                        axis=0,
                    )
                    for s in range(2)
                ],
                axis=1,
            )
            high, low = split(both)
            result = dot(table_w[...], jnp.concatenate([high, high, low], axis=0))
            half[c, p] = result[:, :LANES]
            half[c, p + 1] = result[:, LANES:]

        send_h(c).start()
        keep_h(c).start()

    for copy in tables[:4]:
        copy.wait()
    pl.semaphore_wait(barrier, blocks)

    @pl.loop(0, chunks + AHEAD)
    def _(t):
        @pl.when(t < chunks)
        def _():
            density(t)

        @pl.when(t == AHEAD - 1)
        def _():
            prepare()

        c = t - AHEAD

        @pl.when(c >= 0)
        def _():
            spectrum(c)
            due = c - SLACK + 1

            @pl.when((due > 0) & (lax.rem(due + ratio * TILE, ratio) == 0) & (due // ratio < groups))
            def _():
                gather(due // ratio - 1)

    done = (chunks - SLACK) // ratio

    @pl.loop(max(done, 0), groups - 1)
    def _(g):
        gather(g)

    gather_last()
    filtered(0)

    @pl.loop(0, chunks)
    def _(c):
        @pl.when((lax.rem(c, ratio) == 0) & (c // ratio + 1 < groups))
        def _():
            filtered(c // ratio + 1)

        inverse(c)

    @pl.loop(0, chunks)
    def _(c):
        send_x(c).wait_send()
        arrivals(f_send.at[c]).wait()
        arrivals(b_send.at[c]).wait()
        send_h(c).wait_send()
        keep_h(c).wait()
        send_h(c).wait_recv()


def last_kernel(first, second, table, out):
    planes, nx, count = first.shape[1:]
    a, a_low = split(first[0].reshape(planes * nx, count))
    b, b_low = split(second[0].reshape(planes * nx, count))
    line = dot(jnp.concatenate([a, b, a_low, b_low, a, b], axis=1), table[...])
    out[...] = line.reshape(out.shape)


def fused(orbitals, kweights, occupations, z_basis, z_eigen):
    points, bands, parts, planes, nx, ny = orbitals.shape
    nz = z_basis.shape[0]
    blocks = lax.axis_size("grid")
    kxc = nx // blocks
    step = STEP
    chunks = planes // step
    groups = planes // TILE
    depth = blocks * TILE
    pairs = kxc // 2
    table_x, scaled_x = basis_tables(nx)
    table_y, scaled_y = basis_tables(ny)
    high, low = halves(table_y)
    stack = np.concatenate([high.T, high.T, low.T], axis=0)
    forward_y = np.stack([stack[:, :LANES], stack[:, LANES:]])
    high, low = halves(table_x)
    forward_x = np.concatenate([high, low, high], axis=1)
    high, low = halves(scaled_x.T)
    inverse_x = np.concatenate([high, low, high], axis=1)
    high, low = halves(scaled_y)
    inverse_y = np.concatenate([high, high, low], axis=0)
    wave_y = ((2.0 * np.sin(np.pi * np.arange(ny) / ny)) ** 2).astype(np.float32).reshape(2, LANES)
    wave_x = ((2.0 * np.sin(np.pi * np.arange(nx) / nx)) ** 2).astype(np.float32)

    anywhere = pl.BlockSpec(memory_space=pl.ANY)
    scalars = pl.BlockSpec(memory_space=pltpu.SMEM)
    vector = pl.BlockSpec(memory_space=pltpu.VMEM)
    dma = pltpu.SemaphoreType.DMA
    exchanged = pl.pallas_call(
        fused_kernel,
        out_shape=jax.ShapeDtypeStruct((2, planes, nx, LANES), f32),
        in_specs=[anywhere, scalars, scalars, anywhere, anywhere, anywhere, anywhere, anywhere, vector, scalars],
        out_specs=anywhere,
        scratch_shapes=[
            pltpu.VMEM((SLOTS, points, bands, parts, step, nx, ny), bf16),
            pltpu.VMEM((nx, 2 * ny), bf16),
            pltpu.VMEM((3 * ny, 2 * LANES), bf16),
            pltpu.VMEM((nx, 3 * nx), bf16),
            pltpu.VMEM((nx, 3 * nx), bf16),
            pltpu.VMEM((blocks, planes, nz), f32),
            pltpu.VMEM((1, nz), f32),
            pltpu.VMEM((chunks, step, nx, LANES), f32),
            pltpu.VMEM((chunks, step, nx, LANES), f32),
            pltpu.VMEM((chunks, step, nx, LANES), f32),
            pltpu.VMEM((planes * nx, LANES), f32),
            pltpu.VMEM((groups * depth * kxc, LANES), f32),
            pltpu.VMEM((pairs, nz, 2 * LANES), f32),
            pltpu.VMEM((pairs, nz, 2 * LANES), bf16),
            pltpu.VMEM((pairs, nz, 2 * LANES), bf16),
            pltpu.VMEM((groups, depth, nz), bf16),
            pltpu.VMEM((groups, depth, nz), bf16),
            pltpu.VMEM((groups, nz, 3 * depth), bf16),
            pltpu.VMEM((nz, LANES), f32),
            pltpu.VMEM((planes * nx, LANES), f32),
            pltpu.VMEM((chunks, step, nx, LANES), f32),
            dma((SLOTS,)),
            dma((6,)),
        ]
        + [dma((chunks,))] * 9,
        compiler_params=pltpu.CompilerParams(
            collective_id=0, has_side_effects=True, vmem_limit_bytes=62 * 1024 * 1024
        ),
        name="exchange",
    )(
        orbitals, kweights, occupations, z_basis.reshape(blocks, planes, nz), z_eigen.reshape(1, nz),
        jnp.asarray(forward_y), jnp.asarray(forward_x), jnp.asarray(inverse_x),
        jnp.asarray(wave_y), jnp.asarray(wave_x),
    )
    count = 4
    return pl.pallas_call(
        last_kernel,
        grid=(planes // count,),
        out_shape=jax.ShapeDtypeStruct((planes, nx, ny), f32),
        in_specs=[
            pl.BlockSpec((1, count, nx, LANES), lambda i: (0, i, 0, 0)),
            pl.BlockSpec((1, count, nx, LANES), lambda i: (1, i, 0, 0)),
            pl.BlockSpec((3 * ny, ny), lambda i: (0, 0)),
        ],
        out_specs=pl.BlockSpec((count, nx, ny), lambda i: (i, 0, 0)),
        name="last",
    )(exchanged, exchanged, jnp.asarray(inverse_y))


def real_basis(length):
    position = jnp.arange(length, dtype=jnp.int32)
    product = position[:, None] * position[None, :] % length
    angles = product.astype(jnp.float32) * (2.0 * jnp.pi / length)
    lower = position[:, None] <= length // 2
    table = jnp.where(lower, jnp.cos(angles), jnp.sin(angles))
    edges = (position == 0) | (position == length // 2)
    weights = jnp.where(edges, 1.0, 2.0).astype(jnp.float32) / length
    return (table, table * weights[:, None])


def on_device(orbitals, kweights, occupations, z_basis, z_eigen):
    points, band_count, _, planes, x_length, y_length = orbitals.shape
    z_length = z_basis.shape[0]
    groups = lax.axis_size("kpt")
    blocks = lax.axis_size("grid")
    group = lax.axis_index("kpt")
    ky_count = y_length // groups
    kx_count = x_length // blocks
    step = max(planes // CHUNKS, 1)
    chunks = planes // step
    factor = (kweights[:, None] * occupations).astype(jnp.float32) / (16.0 * points * band_count)
    table_x, scaled_x = real_basis(x_length)
    table_y, scaled_y = real_basis(y_length)

    def part_of(table, shift):
        start = lax.rem(group + shift, groups) * ky_count
        return lax.dynamic_slice_in_dim(table, start, ky_count, 0)

    def shifted_by(shift):
        return [(g, (g + shift) % groups) for g in range(groups)]

    forward_y = [part_of(table_y, shift) for shift in range(groups)]
    inverse_y = [part_of(scaled_y, shift) for shift in range(groups)]
    basis = z_basis.reshape(blocks, planes, z_length)

    projected = None
    for chunk in range(chunks):
        rows = slice(chunk * step, (chunk + 1) * step)
        values = orbitals[:, :, :, rows].astype(jnp.float32)
        density = jnp.sum(factor[:, :, None, None, None, None] * values * values, axis=(0, 1, 2))
        along = jnp.einsum("zxy,ky->zxk", density, forward_y[0], precision=precise)
        for shift in range(1, groups):
            other = jnp.einsum("zxy,ky->zxk", density, forward_y[shift], precision=precise)
            arrived = lax.ppermute(other, "kpt", shifted_by(shift))
            along = along + arrived
        spectrum = jnp.einsum("jx,zxk->zjk", table_x, along, precision=precise)
        column = lax.all_to_all(
            spectrum.reshape(step, blocks, kx_count, ky_count), "grid", split_axis=1, concat_axis=0, tiled=True
        ).reshape(blocks * step, kx_count, ky_count)
        z_rows = basis[:, rows].reshape(blocks * step, z_length)
        term = jnp.einsum("zj,zab->jab", z_rows, column, precision=precise)
        projected = term if projected is None else projected + term

    wave_x = (lax.axis_index("grid") * kx_count + jnp.arange(kx_count, dtype=jnp.int32)).astype(jnp.float32)
    wave_y = (group * ky_count + jnp.arange(ky_count, dtype=jnp.int32)).astype(jnp.float32)
    shift_x = 2.0 * jnp.sin(jnp.pi * wave_x / x_length)
    shift_y = 2.0 * jnp.sin(jnp.pi * wave_y / y_length)
    shifted = shift_x[:, None] ** 2 + shift_y[None, :] ** 2
    scaled = projected * (1.0 / (z_eigen[:, None, None] + shifted[None]))

    outputs = []
    for chunk in range(chunks):
        rows = slice(chunk * step, (chunk + 1) * step)
        z_rows = basis[:, rows].reshape(blocks * step, z_length)
        filtered = jnp.einsum("zj,jab->zab", z_rows, scaled, precision=precise)
        modes = lax.all_to_all(
            filtered.reshape(blocks, step, kx_count, ky_count), "grid", split_axis=0, concat_axis=0, tiled=True
        )
        half = jnp.einsum(
            "jx,zjk->zxk",
            scaled_x,
            modes.transpose(1, 0, 2, 3).reshape(step, x_length, ky_count),
            precision=precise,
        )
        total = jnp.einsum("zxk,ky->zxy", half, inverse_y[0], precision=precise)
        for shift in range(1, groups):
            arrived = lax.ppermute(half, "kpt", shifted_by(groups - shift))
            total = total + jnp.einsum("zxk,ky->zxy", arrived, inverse_y[shift], precision=precise)
        outputs.append(total)
    return jnp.concatenate(outputs, axis=0)


def solution(mesh):
    groups, blocks = mesh.shape["kpt"], mesh.shape["grid"]
    specs = dict(
        mesh=mesh,
        in_specs=(P("kpt", None, None, "grid", None, None), P("kpt"), P("kpt", None), P(), P()),
        out_specs=P("grid", None, None),
        check_vma=False,
    )
    plain = jax.shard_map(on_device, **specs)
    kernels = jax.shard_map(fused, **specs)

    def step(orbitals, *rest):
        _, _, _, nz, nx, ny = orbitals.shape
        fits = groups == 2 and ny == 2 * LANES and nx % (TILE * blocks) == 0 and nz % (TILE * blocks) == 0
        return (kernels if fits else plain)(orbitals, *rest)

    return step
```

```python
import jax
import jax.numpy as jnp
import numpy as np
from jax import lax
from jax.experimental import pallas as pl
from jax.experimental.pallas import tpu as pltpu
from jax.sharding import PartitionSpec as P


precise = lax.Precision.HIGH
CHUNKS = 4

MESH = pl.DeviceIdType.MESH
LANES = 128
TILE = 8
BITE = 2
STEP = 2
SLOTS = 3
LEAD = 3
PACE = 1
LATE = 4
EARLY = 2
WINDOW = 3
MIDDLE = 8
REST = 1
LATER = 4
bf16 = jnp.bfloat16
f32 = jnp.float32


def basis_tables(length):
    position = np.arange(length)
    angles = (position[:, None] * position[None, :] % length) * (2.0 * np.pi / length)
    table = np.where(position[:, None] <= length // 2, np.cos(angles), np.sin(angles))
    edges = (position == 0) | (position == length // 2)
    scaled = table * (np.where(edges, 1.0, 2.0) / length)[:, None]
    return table, scaled


def halves(table):
    high = table.astype(bf16)
    low = (table - high.astype(np.float64)).astype(bf16)
    return high, low


def split(value):
    high = value.astype(bf16)
    return high, (value - high.astype(f32)).astype(bf16)


def dot(left, right):
    return jnp.dot(left, right, preferred_element_type=f32)


def fused_kernel(
    orbitals, kweights, occupations, basis, eigen, forward_y, forward_x, inverse_x, wave_y, wave_x,
    line_out,
    block, rows, table_y, table_x, table_w, basis_rows, eigen_row, own, leaving, joined, column, projected,
    scaled_high, scaled_low, basis_high, basis_low, basis_turned, eigen_column, modes, others, line,
    load_sem, table_sem, x_send, x_recv, f_send, f_recv, b_send, b_recv, h_send, h_recv, keep_sem,
):
    points, bands, parts, planes, nx, ny = orbitals.shape
    blocks = lax.axis_size("grid")
    chunks = planes // STEP
    groups = planes // TILE
    ratio = TILE // STEP
    cuts = nx // (blocks * TILE)
    items = cuts * chunks
    depth = blocks * TILE
    pairs = TILE // 2
    share = STEP * TILE
    nz = basis.shape[0] * basis.shape[1]
    bites = planes // BITE
    per = STEP // BITE
    side = lax.axis_index("kpt")
    other = 1 - side
    me = lax.axis_index("grid")

    barrier = pltpu.get_barrier_semaphore()
    pl.semaphore_signal(barrier, inc=1, device_id={"kpt": other}, device_id_type=MESH)

    @pl.loop(1, blocks)
    def _(i):
        pl.semaphore_signal(barrier, inc=1, device_id={"grid": lax.rem(me + i, blocks)}, device_id_type=MESH)

    def load(b):
        slot = lax.rem(b, SLOTS)
        return pltpu.make_async_copy(
            orbitals.at[:, :, :, pl.ds(b * BITE, BITE)], block.at[slot], load_sem.at[slot]
        )

    load(0).start()
    tables = [
        pltpu.make_async_copy(forward_y.at[side], table_y, table_sem.at[0]),
        pltpu.make_async_copy(forward_x, table_x, table_sem.at[1]),
        pltpu.make_async_copy(inverse_x, table_w, table_sem.at[2]),
        pltpu.make_async_copy(basis, basis_rows, table_sem.at[3]),
        pltpu.make_async_copy(eigen, eigen_row, table_sem.at[4]),
    ]
    for copy in tables[:2]:
        copy.start()

    def part_of(e, d):
        return pl.ds(pl.multiple_of((e * blocks + d) * share, TILE), share)

    def place_of(e, d):
        c = lax.rem(e, chunks)
        first = ((e // chunks * groups + c // ratio) * blocks + d) * TILE + lax.rem(c, ratio) * STEP
        return pl.ds(pl.multiple_of(first * TILE, TILE), share)

    def whole_of(e):
        return pl.ds(pl.multiple_of(e * (blocks * share), TILE), blocks * share)

    def across_kpt(source, target, e, send, recv):
        return pltpu.make_async_remote_copy(
            src_ref=source.at[whole_of(e)], dst_ref=target.at[whole_of(e)],
            send_sem=send.at[e], recv_sem=recv.at[e], device_id={"kpt": other}, device_id_type=MESH,
        )

    def send_x(e):
        return across_kpt(leaving, joined, e, x_send, x_recv)

    def send_h(e):
        return across_kpt(modes, others, e, h_send, h_recv)

    def send_f(e, i):
        to = lax.rem(me + i, blocks)
        return pltpu.make_async_remote_copy(
            src_ref=own.at[part_of(e, to)], dst_ref=column.at[place_of(e, me)],
            send_sem=f_send.at[e], recv_sem=f_recv.at[e], device_id={"grid": to}, device_id_type=MESH,
        )

    def send_b(e, i):
        to = lax.rem(me + i, blocks)
        return pltpu.make_async_remote_copy(
            src_ref=column.at[place_of(e, to)], dst_ref=modes.at[part_of(e, me)],
            send_sem=b_send.at[e], recv_sem=b_recv.at[e], device_id={"grid": to}, device_id_type=MESH,
        )

    def arrivals(sem):
        whole = column.at[pl.ds(0, (blocks - 1) * share)]
        return pltpu.make_async_copy(whole, whole, sem)

    def density(b):
        slot = lax.rem(b, SLOTS)
        load(b).wait()

        @pl.when(b == 0)
        def _():
            for later in range(1, SLOTS):
                load(later).start()
            for copy in tables[2:]:
                copy.start()

        strip = 32
        factors = [
            [(kweights[k] * occupations[k, n]).astype(f32) / (16.0 * points * bands) for n in range(bands)]
            for k in range(points)
        ]

        @pl.loop(0, BITE * nx // strip)
        def _(r):
            p = r // (nx // strip)
            where = pl.ds(pl.multiple_of(lax.rem(r, nx // strip) * strip, strip), strip)
            target = pl.ds(pl.multiple_of(r * strip, strip), strip)
            total = None
            for k in range(points):
                for n in range(bands):
                    square = None
                    for part in range(parts):
                        value = block[slot, k, n, part, p, where, :].astype(f32)
                        square = value * value if square is None else square + value * value
                    term = factors[k][n] * square
                    total = term if total is None else total + term
            high, low = split(total)
            rows[target, pl.ds(0, ny)] = high
            rows[target, pl.ds(ny, ny)] = low

        @pl.when(b + SLOTS < bites)
        def _():
            load(b + SLOTS).start()

        along = dot(rows[...], table_y[pl.ds(0, 2 * ny), :]) + dot(
            rows[:, pl.ds(0, ny)], table_y[pl.ds(2 * ny, ny), :]
        )
        for p in range(BITE):
            high, low = split(along[p * nx : (p + 1) * nx])
            result = dot(table_x[...], jnp.concatenate([high, high, low], axis=0))
            c = b // per
            q = lax.rem(b, per) * BITE + p
            for h in range(cuts):
                for d in range(blocks):
                    first = (((h * chunks + c) * blocks + d) * STEP + q) * TILE
                    where = pl.ds(pl.multiple_of(first, TILE), TILE)
                    taken = result[(h * blocks + d) * TILE : (h * blocks + d + 1) * TILE]
                    leaving[where, :] = taken[:, :LANES]
                    own[where, :] = taken[:, LANES:]

    def spectrum(e):
        send_x(e).wait_recv()
        own[whole_of(e), :] += joined[whole_of(e), :]
        column[place_of(e, me), :] = own[part_of(e, me), :]

        @pl.when(e >= items - EARLY)
        def _():
            arrivals(f_recv.at[e - 1]).wait()

        @pl.loop(1, blocks)
        def _(i):
            send_f(e, i).start()

    def prepare():
        for copy in tables[2:]:
            copy.wait()

        @pl.loop(0, groups)
        def _(g):
            taken = basis_rows[:, pl.ds(pl.multiple_of(g * TILE, TILE), TILE), :].reshape(depth, nz)
            high, low = split(taken)
            basis_high[g] = high
            basis_low[g] = low
            high, low = split(taken.T)
            basis_turned[g, :, pl.ds(0, depth)] = high
            basis_turned[g, :, pl.ds(depth, depth)] = high
            basis_turned[g, :, pl.ds(2 * depth, depth)] = low

        eigen_column[...] = jnp.broadcast_to(eigen_row[...], (LANES, nz)).T

    def start_of(h, g, q):
        return (h * groups + g) * (depth * TILE) + 2 * q

    def term(h, g, q):
        start = start_of(h, g, q)
        both = jnp.concatenate(
            [column[pl.ds(start, depth, stride=TILE), :], column[pl.ds(start + 1, depth, stride=TILE), :]], axis=1
        )
        high, low = split(both)
        return dot(basis_turned[g], jnp.concatenate([high, low, high], axis=0))

    def wait_f(h, g):
        for r in range(ratio):
            e = h * chunks + g * ratio + r

            @pl.when((e < items - EARLY - 1) | (e == items - 1))
            def _():
                arrivals(f_recv.at[e]).wait()

    def gather(h, g):
        wait_f(h, g)

        @pl.loop(0, pairs)
        def _(q):
            projected[q] = jnp.where(g > 0, projected[q], 0.0) + term(h, g, q)

    def gather_last(h):
        g = groups - 1
        wait_f(h, g)
        across = wave_y[pl.ds(side, 1), :]

        @pl.loop(0, pairs)
        def _(q):
            total = term(h, g, q)
            if groups > 1:
                total = total + projected[q]
            for s in range(2):
                along = wave_x[(me * cuts + h) * TILE + 2 * q + s]
                value = total[:, s * LANES : (s + 1) * LANES] / (eigen_column[...] + (along + across))
                high, low = split(value)
                scaled_high[q, :, pl.ds(s * LANES, LANES)] = high
                scaled_low[q, :, pl.ds(s * LANES, LANES)] = low

    def filtered(h, g):
        @pl.loop(0, pairs)
        def _(q):
            result = (
                dot(basis_high[g], scaled_high[q])
                + dot(basis_high[g], scaled_low[q])
                + dot(basis_low[g], scaled_high[q])
            )
            start = start_of(h, g, q)
            column[pl.ds(start, depth, stride=TILE), :] = result[:, :LANES]
            column[pl.ds(start + 1, depth, stride=TILE), :] = result[:, LANES:]

        for r in range(ratio):
            e = h * chunks + g * ratio + r
            modes[part_of(e, me), :] = column[place_of(e, me), :]

    def give_back(e):
        @pl.loop(1, blocks)
        def _(i):
            send_b(e, i).start()

    def hand_over(e):
        arrivals(b_recv.at[e]).wait()
        send_h(e).start()

    def keep(c, s):
        slot = lax.rem(c, 2)
        return pltpu.make_async_copy(
            line.at[slot, s], line_out.at[side if s == 0 else other, pl.ds(c * STEP, STEP)], keep_sem.at[slot, s]
        )

    def inverse(c):
        for h in range(cuts):
            send_h(h * chunks + c).wait_recv()

        @pl.when(c >= 2)
        def _():
            for s in range(2):
                keep(c - 2, s).wait()

        slot = lax.rem(c, 2)

        @pl.loop(0, STEP)
        def _(p):
            both = jnp.concatenate(
                [
                    jnp.concatenate(
                        [
                            source[pl.ds(pl.multiple_of((((h * chunks + c) * blocks + d) * STEP + p) * TILE, TILE), TILE), :]
                            for h in range(cuts)
                            for d in range(blocks)
                        ],
                        axis=0,
                    )
                    for source in (modes, others)
                ],
                axis=1,
            )
            high, low = split(both)
            result = dot(table_w[...], jnp.concatenate([high, high, low], axis=0))
            line[slot, 0, p] = result[:, :LANES]
            line[slot, 1, p] = result[:, LANES:]

        for s in range(2):
            keep(c, s).start()

    for copy in tables[:2]:
        copy.wait()

    @pl.loop(0, bites)
    def _(b):
        density(b)

        @pl.when(b == 0)
        def _():
            pl.semaphore_wait(barrier, blocks)

        @pl.when(lax.rem(b, per) == per - 1)
        def _():
            send_x(b // per).start()

        @pl.when((b >= LEAD) & (lax.rem(b - LEAD, PACE) == 0))
        def _():
            spectrum((b - LEAD) // PACE)

    first = (bites - 1 - LEAD) // PACE + 1

    @pl.loop(chunks, items)
    def _(e):
        send_x(e).start()

    prepare()

    last = cuts - 1
    base = last * chunks + ratio + LATER - 1

    @pl.loop(first, items)
    def _(e):
        spectrum(e)
        at = chunks + LATE - groups

        @pl.when((e >= at) & (e < at + groups - 1))
        def _():
            gather(0, e - at)

        @pl.when(e == at + groups - 1)
        def _():
            gather_last(0)

        @pl.when((e >= at + groups) & (e < at + 2 * groups))
        def _():
            filtered(0, e - at - groups)

        @pl.when((e >= base) & (lax.rem(e - base + ratio * items, ratio) == 0))
        def _():
            gather(last, (e - base) // ratio)

        k = e - (items - EARLY)

        @pl.when(k >= 1)
        def _():
            hand_over(k - 1)

        @pl.when(k >= 0)
        def _():
            give_back(k)

    for e in range(EARLY, EARLY + WINDOW - 1):
        give_back(e)

    done = (items - 1 - base) // ratio + 1

    @pl.loop(EARLY - 1, items)
    def _(e):
        ahead = e + WINDOW
        hand_over(e)

        @pl.when(ahead < items)
        def _():
            give_back(ahead)

        @pl.when((e >= REST) & (e - REST + done < groups - 1))
        def _():
            gather(last, e - REST + done)

        @pl.when(e == MIDDLE)
        def _():
            gather_last(last)

        after = ahead + 1 - last * chunks

        @pl.when((after >= 0) & (after < chunks) & (lax.rem(after + items * ratio, ratio) == 0))
        def _():
            filtered(last, after // ratio)

        @pl.when(e > last * chunks)
        def _():
            inverse(e - last * chunks - 1)

    inverse(chunks - 1)

    for c in (chunks - 2, chunks - 1):
        for s in range(2):
            keep(c, s).wait()

    @pl.loop(0, items)
    def _(e):
        send_x(e).wait_send()
        arrivals(f_send.at[e]).wait()
        arrivals(b_send.at[e]).wait()
        send_h(e).wait_send()


def last_kernel(first, second, table, out):
    planes, nx, count = first.shape[1:]
    a, a_low = split(first[0].reshape(planes * nx, count))
    b, b_low = split(second[0].reshape(planes * nx, count))
    line = dot(jnp.concatenate([a, b, a_low, b_low, a, b], axis=1), table[...])
    out[...] = line.reshape(out.shape)


def fused(orbitals, kweights, occupations, z_basis, z_eigen):
    points, bands, parts, planes, nx, ny = orbitals.shape
    nz = z_basis.shape[0]
    blocks = lax.axis_size("grid")
    chunks = planes // STEP
    groups = planes // TILE
    cuts = nx // (blocks * TILE)
    items = cuts * chunks
    depth = blocks * TILE
    pairs = TILE // 2
    order = np.arange(nx).reshape(blocks, cuts, TILE).transpose(1, 0, 2).reshape(nx)
    table_x, scaled_x = basis_tables(nx)
    table_y, scaled_y = basis_tables(ny)
    high, low = halves(table_y)
    stack = np.concatenate([high.T, high.T, low.T], axis=0)
    forward_y = np.stack([np.roll(stack, LANES, axis=1), stack])
    high, low = halves(table_x[order])
    forward_x = np.concatenate([high, low, high], axis=1)
    high, low = halves(scaled_x[order].T)
    inverse_x = np.concatenate([high, low, high], axis=1)
    high, low = halves(scaled_y)
    inverse_y = np.concatenate([high, high, low], axis=0)
    wave_y = ((2.0 * np.sin(np.pi * np.arange(ny) / ny)) ** 2).astype(np.float32).reshape(2, LANES)
    wave_x = ((2.0 * np.sin(np.pi * np.arange(nx) / nx)) ** 2).astype(np.float32)

    anywhere = pl.BlockSpec(memory_space=pl.ANY)
    scalars = pl.BlockSpec(memory_space=pltpu.SMEM)
    vector = pl.BlockSpec(memory_space=pltpu.VMEM)
    dma = pltpu.SemaphoreType.DMA
    exchanged = pl.pallas_call(
        fused_kernel,
        out_shape=jax.ShapeDtypeStruct((2, planes, nx, LANES), f32),
        in_specs=[anywhere, scalars, scalars, anywhere, anywhere, anywhere, anywhere, anywhere, vector, scalars],
        out_specs=anywhere,
        scratch_shapes=[
            pltpu.VMEM((SLOTS, points, bands, parts, BITE, nx, ny), bf16),
            pltpu.VMEM((BITE * nx, 2 * ny), bf16),
            pltpu.VMEM((3 * ny, 2 * LANES), bf16),
            pltpu.VMEM((nx, 3 * nx), bf16),
            pltpu.VMEM((nx, 3 * nx), bf16),
            pltpu.VMEM((blocks, planes, nz), f32),
            pltpu.VMEM((1, nz), f32),
            pltpu.VMEM((planes * nx, LANES), f32),
            pltpu.VMEM((planes * nx, LANES), f32),
            pltpu.VMEM((planes * nx, LANES), f32),
            pltpu.VMEM((planes * nx, LANES), f32),
            pltpu.VMEM((pairs, nz, 2 * LANES), f32),
            pltpu.VMEM((pairs, nz, 2 * LANES), bf16),
            pltpu.VMEM((pairs, nz, 2 * LANES), bf16),
            pltpu.VMEM((groups, depth, nz), bf16),
            pltpu.VMEM((groups, depth, nz), bf16),
            pltpu.VMEM((groups, nz, 3 * depth), bf16),
            pltpu.VMEM((nz, LANES), f32),
            pltpu.VMEM((planes * nx, LANES), f32),
            pltpu.VMEM((planes * nx, LANES), f32),
            pltpu.VMEM((2, 2, STEP, nx, LANES), f32),
            dma((SLOTS,)),
            dma((5,)),
        ]
        + [dma((items,))] * 8
        + [dma((2, 2))],
        compiler_params=pltpu.CompilerParams(
            collective_id=0, has_side_effects=True, vmem_limit_bytes=62 * 1024 * 1024
        ),
        name="exchange",
    )(
        orbitals, kweights, occupations, z_basis.reshape(blocks, planes, nz), z_eigen.reshape(1, nz),
        jnp.asarray(forward_y), jnp.asarray(forward_x), jnp.asarray(inverse_x),
        jnp.asarray(wave_y), jnp.asarray(wave_x),
    )
    count = TILE
    return pl.pallas_call(
        last_kernel,
        grid=(planes // count,),
        out_shape=jax.ShapeDtypeStruct((planes, nx, ny), f32),
        in_specs=[
            pl.BlockSpec((1, count, nx, LANES), lambda i: (0, i, 0, 0)),
            pl.BlockSpec((1, count, nx, LANES), lambda i: (1, i, 0, 0)),
            pl.BlockSpec((3 * ny, ny), lambda i: (0, 0)),
        ],
        out_specs=pl.BlockSpec((count, nx, ny), lambda i: (i, 0, 0)),
        name="last",
    )(exchanged, exchanged, jnp.asarray(inverse_y))


def real_basis(length):
    position = jnp.arange(length, dtype=jnp.int32)
    product = position[:, None] * position[None, :] % length
    angles = product.astype(jnp.float32) * (2.0 * jnp.pi / length)
    lower = position[:, None] <= length // 2
    table = jnp.where(lower, jnp.cos(angles), jnp.sin(angles))
    edges = (position == 0) | (position == length // 2)
    weights = jnp.where(edges, 1.0, 2.0).astype(jnp.float32) / length
    return (table, table * weights[:, None])


def on_device(orbitals, kweights, occupations, z_basis, z_eigen):
    points, band_count, _, planes, x_length, y_length = orbitals.shape
    z_length = z_basis.shape[0]
    groups = lax.axis_size("kpt")
    blocks = lax.axis_size("grid")
    group = lax.axis_index("kpt")
    ky_count = y_length // groups
    kx_count = x_length // blocks
    step = max(planes // CHUNKS, 1)
    chunks = planes // step
    factor = (kweights[:, None] * occupations).astype(jnp.float32) / (16.0 * points * band_count)
    table_x, scaled_x = real_basis(x_length)
    table_y, scaled_y = real_basis(y_length)

    def part_of(table, shift):
        start = lax.rem(group + shift, groups) * ky_count
        return lax.dynamic_slice_in_dim(table, start, ky_count, 0)

    def shifted_by(shift):
        return [(g, (g + shift) % groups) for g in range(groups)]

    forward_y = [part_of(table_y, shift) for shift in range(groups)]
    inverse_y = [part_of(scaled_y, shift) for shift in range(groups)]
    basis = z_basis.reshape(blocks, planes, z_length)

    projected = None
    for chunk in range(chunks):
        rows = slice(chunk * step, (chunk + 1) * step)
        values = orbitals[:, :, :, rows].astype(jnp.float32)
        density = jnp.sum(factor[:, :, None, None, None, None] * values * values, axis=(0, 1, 2))
        along = jnp.einsum("zxy,ky->zxk", density, forward_y[0], precision=precise)
        for shift in range(1, groups):
            other = jnp.einsum("zxy,ky->zxk", density, forward_y[shift], precision=precise)
            arrived = lax.ppermute(other, "kpt", shifted_by(shift))
            along = along + arrived
        spectrum = jnp.einsum("jx,zxk->zjk", table_x, along, precision=precise)
        column = lax.all_to_all(
            spectrum.reshape(step, blocks, kx_count, ky_count), "grid", split_axis=1, concat_axis=0, tiled=True
        ).reshape(blocks * step, kx_count, ky_count)
        z_rows = basis[:, rows].reshape(blocks * step, z_length)
        term = jnp.einsum("zj,zab->jab", z_rows, column, precision=precise)
        projected = term if projected is None else projected + term

    wave_x = (lax.axis_index("grid") * kx_count + jnp.arange(kx_count, dtype=jnp.int32)).astype(jnp.float32)
    wave_y = (group * ky_count + jnp.arange(ky_count, dtype=jnp.int32)).astype(jnp.float32)
    shift_x = 2.0 * jnp.sin(jnp.pi * wave_x / x_length)
    shift_y = 2.0 * jnp.sin(jnp.pi * wave_y / y_length)
    shifted = shift_x[:, None] ** 2 + shift_y[None, :] ** 2
    scaled = projected * (1.0 / (z_eigen[:, None, None] + shifted[None]))

    outputs = []
    for chunk in range(chunks):
        rows = slice(chunk * step, (chunk + 1) * step)
        z_rows = basis[:, rows].reshape(blocks * step, z_length)
        filtered = jnp.einsum("zj,jab->zab", z_rows, scaled, precision=precise)
        modes = lax.all_to_all(
            filtered.reshape(blocks, step, kx_count, ky_count), "grid", split_axis=0, concat_axis=0, tiled=True
        )
        half = jnp.einsum(
            "jx,zjk->zxk",
            scaled_x,
            modes.transpose(1, 0, 2, 3).reshape(step, x_length, ky_count),
            precision=precise,
        )
        total = jnp.einsum("zxk,ky->zxy", half, inverse_y[0], precision=precise)
        for shift in range(1, groups):
            arrived = lax.ppermute(half, "kpt", shifted_by(groups - shift))
            total = total + jnp.einsum("zxk,ky->zxy", arrived, inverse_y[shift], precision=precise)
        outputs.append(total)
    return jnp.concatenate(outputs, axis=0)


def solution(mesh):
    groups, blocks = mesh.shape["kpt"], mesh.shape["grid"]
    specs = dict(
        mesh=mesh,
        in_specs=(P("kpt", None, None, "grid", None, None), P("kpt"), P("kpt", None), P(), P()),
        out_specs=P("grid", None, None),
        check_vma=False,
    )
    plain = jax.shard_map(on_device, **specs)
    kernels = jax.shard_map(fused, **specs)

    def step(orbitals, *rest):
        _, _, _, nz, nx, ny = orbitals.shape
        fits = groups == 2 and ny == 2 * LANES and nx == 2 * TILE * blocks and nz % (TILE * blocks) == 0
        return (kernels if fits else plain)(orbitals, *rest)

    return step
```

```python
import jax
import jax.numpy as jnp
import numpy as np
from jax import lax
from jax.experimental import pallas as pl
from jax.experimental.pallas import tpu as pltpu
from jax.sharding import PartitionSpec as P


precise = lax.Precision.HIGH
CHUNKS = 4

MESH = pl.DeviceIdType.MESH
LANES = 128
TILE = 8
BITE = 2
PART = 4
STEP = 2
SLOTS = 3
LEAD = 3
PACE = 1
LATE = 4
EARLY = 2
WINDOW = 3
MIDDLE = 8
REST = 1
LATER = 4
bf16 = jnp.bfloat16
f32 = jnp.float32


def basis_tables(length):
    position = np.arange(length)
    angles = (position[:, None] * position[None, :] % length) * (2.0 * np.pi / length)
    table = np.where(position[:, None] <= length // 2, np.cos(angles), np.sin(angles))
    edges = (position == 0) | (position == length // 2)
    scaled = table * (np.where(edges, 1.0, 2.0) / length)[:, None]
    return table, scaled


def halves(table):
    high = table.astype(bf16)
    low = (table - high.astype(np.float64)).astype(bf16)
    return high, low


def split(value):
    high = value.astype(bf16)
    return high, (value - high.astype(f32)).astype(bf16)


def dot(left, right):
    return jnp.dot(left, right, preferred_element_type=f32)


def fused_kernel(
    orbitals, kweights, occupations, basis, eigen, forward_y, forward_x, inverse_x, wave_y, wave_x,
    line_out,
    block, rows, table_y, table_x, table_w, basis_rows, eigen_row, own, leaving, joined, column, projected,
    scaled_high, scaled_low, basis_high, basis_low, basis_turned, eigen_column, modes, others, line,
    load_sem, table_sem, x_send, x_recv, f_send, f_recv, b_send, b_recv, h_send, h_recv, keep_sem,
):
    points, bands, parts, planes, nx, ny = orbitals.shape
    blocks = lax.axis_size("grid")
    chunks = planes // STEP
    groups = planes // TILE
    ratio = TILE // STEP
    cuts = nx // (blocks * TILE)
    items = cuts * chunks
    depth = blocks * TILE
    pairs = TILE // 2
    share = STEP * TILE
    nz = basis.shape[0] * basis.shape[1]
    bites = planes // BITE
    per = STEP // BITE
    side = lax.axis_index("kpt")
    other = 1 - side
    me = lax.axis_index("grid")

    barrier = pltpu.get_barrier_semaphore()
    pl.semaphore_signal(barrier, inc=1, device_id={"kpt": other}, device_id_type=MESH)

    @pl.loop(1, blocks)
    def _(i):
        pl.semaphore_signal(barrier, inc=1, device_id={"grid": lax.rem(me + i, blocks)}, device_id_type=MESH)

    def load(b):
        slot = lax.rem(b, SLOTS)
        return pltpu.make_async_copy(
            orbitals.at[:, :, :, pl.ds(b * BITE, BITE)], block.at[slot], load_sem.at[slot]
        )

    load(0).start()
    tables = [
        pltpu.make_async_copy(forward_y.at[side], table_y, table_sem.at[0]),
        pltpu.make_async_copy(forward_x, table_x, table_sem.at[1]),
        pltpu.make_async_copy(inverse_x, table_w, table_sem.at[2]),
        pltpu.make_async_copy(basis, basis_rows, table_sem.at[3]),
        pltpu.make_async_copy(eigen, eigen_row, table_sem.at[4]),
    ]
    for copy in tables[:2]:
        copy.start()

    def part_of(e, d):
        return pl.ds(pl.multiple_of((e * blocks + d) * share, TILE), share)

    def place_of(e, d):
        c = lax.rem(e, chunks)
        first = ((e // chunks * groups + c // ratio) * blocks + d) * TILE + lax.rem(c, ratio) * STEP
        return pl.ds(pl.multiple_of(first * TILE, TILE), share)

    def whole_of(e):
        return pl.ds(pl.multiple_of(e * (blocks * share), TILE), blocks * share)

    def across_kpt(source, target, e, send, recv):
        return pltpu.make_async_remote_copy(
            src_ref=source.at[whole_of(e)], dst_ref=target.at[whole_of(e)],
            send_sem=send.at[e], recv_sem=recv.at[e], device_id={"kpt": other}, device_id_type=MESH,
        )

    def send_x(e):
        return across_kpt(leaving, joined, e, x_send, x_recv)

    def send_h(e):
        return across_kpt(modes, others, e, h_send, h_recv)

    def send_f(e, i):
        to = lax.rem(me + i, blocks)
        return pltpu.make_async_remote_copy(
            src_ref=own.at[part_of(e, to)], dst_ref=column.at[place_of(e, me)],
            send_sem=f_send.at[e], recv_sem=f_recv.at[e], device_id={"grid": to}, device_id_type=MESH,
        )

    def send_b(e, i):
        to = lax.rem(me + i, blocks)
        return pltpu.make_async_remote_copy(
            src_ref=column.at[place_of(e, to)], dst_ref=modes.at[part_of(e, me)],
            send_sem=b_send.at[e], recv_sem=b_recv.at[e], device_id={"grid": to}, device_id_type=MESH,
        )

    def arrivals(sem):
        whole = column.at[pl.ds(0, (blocks - 1) * share)]
        return pltpu.make_async_copy(whole, whole, sem)

    def density(b):
        slot = lax.rem(b, SLOTS)
        load(b).wait()

        @pl.when(b == 0)
        def _():
            for later in range(1, SLOTS):
                load(later).start()
            for copy in tables[2:]:
                copy.start()

        strip = 32
        factors = [
            [(kweights[k] * occupations[k, n]).astype(f32) / (16.0 * points * bands) for n in range(bands)]
            for k in range(points)
        ]

        @pl.loop(0, BITE * nx // strip)
        def _(r):
            p = r // (nx // strip)
            where = pl.ds(pl.multiple_of(lax.rem(r, nx // strip) * strip, strip), strip)
            target = pl.ds(pl.multiple_of(r * strip, strip), strip)
            total = None
            for k in range(points):
                for n in range(bands):
                    square = None
                    for part in range(parts):
                        value = block[slot, k, n, part, p, where, :].astype(f32)
                        square = value * value if square is None else square + value * value
                    term = factors[k][n] * square
                    total = term if total is None else total + term
            high, low = split(total)
            rows[target, pl.ds(0, ny)] = high
            rows[target, pl.ds(ny, ny)] = low

        @pl.when(b + SLOTS < bites)
        def _():
            load(b + SLOTS).start()

        along = dot(rows[...], table_y[pl.ds(0, 2 * ny), :]) + dot(
            rows[:, pl.ds(0, ny)], table_y[pl.ds(2 * ny, ny), :]
        )
        for p in range(BITE):
            high, low = split(along[p * nx : (p + 1) * nx])
            result = dot(table_x[...], jnp.concatenate([high, high, low], axis=0))
            c = b // per
            q = lax.rem(b, per) * BITE + p
            for h in range(cuts):
                for d in range(blocks):
                    first = (((h * chunks + c) * blocks + d) * STEP + q) * TILE
                    where = pl.ds(pl.multiple_of(first, TILE), TILE)
                    taken = result[(h * blocks + d) * TILE : (h * blocks + d + 1) * TILE]
                    leaving[where, :] = taken[:, :LANES]
                    own[where, :] = taken[:, LANES:]

    def spectrum(e):
        send_x(e).wait_recv()
        own[whole_of(e), :] += joined[whole_of(e), :]
        column[place_of(e, me), :] = own[part_of(e, me), :]

        @pl.when(e >= items - EARLY)
        def _():
            arrivals(f_recv.at[e - 1]).wait()

        @pl.loop(1, blocks)
        def _(i):
            send_f(e, i).start()

    def prepare():
        for copy in tables[2:]:
            copy.wait()

        @pl.loop(0, groups)
        def _(g):
            taken = basis_rows[:, pl.ds(pl.multiple_of(g * TILE, TILE), TILE), :].reshape(depth, nz)
            high, low = split(taken)
            basis_high[g] = high
            basis_low[g] = low
            high, low = split(taken.T)
            basis_turned[g, :, pl.ds(0, depth)] = high
            basis_turned[g, :, pl.ds(depth, depth)] = high
            basis_turned[g, :, pl.ds(2 * depth, depth)] = low

        eigen_column[...] = jnp.broadcast_to(eigen_row[...], (LANES, nz)).T

    def start_of(h, g, q):
        return (h * groups + g) * (depth * TILE) + 2 * q

    def term(h, g, q):
        start = start_of(h, g, q)
        both = jnp.concatenate(
            [column[pl.ds(start, depth, stride=TILE), :], column[pl.ds(start + 1, depth, stride=TILE), :]], axis=1
        )
        high, low = split(both)
        return dot(basis_turned[g], jnp.concatenate([high, low, high], axis=0))

    def wait_f(h, g):
        for r in range(ratio):
            e = h * chunks + g * ratio + r

            @pl.when((e < items - EARLY - 1) | (e == items - 1))
            def _():
                arrivals(f_recv.at[e]).wait()

    def gather(h, g):
        wait_f(h, g)

        @pl.loop(0, pairs)
        def _(q):
            projected[q] = jnp.where(g > 0, projected[q], 0.0) + term(h, g, q)

    def gather_last(h):
        g = groups - 1
        wait_f(h, g)
        across = wave_y[pl.ds(side, 1), :]

        @pl.loop(0, pairs)
        def _(q):
            total = term(h, g, q)
            if groups > 1:
                total = total + projected[q]
            for s in range(2):
                along = wave_x[(me * cuts + h) * TILE + 2 * q + s]
                value = total[:, s * LANES : (s + 1) * LANES] / (eigen_column[...] + (along + across))
                high, low = split(value)
                scaled_high[q, :, pl.ds(s * LANES, LANES)] = high
                scaled_low[q, :, pl.ds(s * LANES, LANES)] = low

    def filtered(h, g):
        @pl.loop(0, pairs)
        def _(q):
            result = (
                dot(basis_high[g], scaled_high[q])
                + dot(basis_high[g], scaled_low[q])
                + dot(basis_low[g], scaled_high[q])
            )
            start = start_of(h, g, q)
            column[pl.ds(start, depth, stride=TILE), :] = result[:, :LANES]
            column[pl.ds(start + 1, depth, stride=TILE), :] = result[:, LANES:]

        for r in range(ratio):
            e = h * chunks + g * ratio + r
            modes[part_of(e, me), :] = column[place_of(e, me), :]

    def give_back(e):
        @pl.loop(1, blocks)
        def _(i):
            send_b(e, i).start()

    def hand_over(e):
        arrivals(b_recv.at[e]).wait()
        send_h(e).start()

    def keep(c, s):
        slot = lax.rem(c, 2)
        return pltpu.make_async_copy(
            line.at[slot, s], line_out.at[side if s == 0 else other, pl.ds(c * STEP, STEP)], keep_sem.at[slot, s]
        )

    def inverse(c):
        for h in range(cuts):
            send_h(h * chunks + c).wait_recv()

        @pl.when(c >= 2)
        def _():
            for s in range(2):
                keep(c - 2, s).wait()

        slot = lax.rem(c, 2)

        @pl.loop(0, STEP)
        def _(p):
            both = jnp.concatenate(
                [
                    jnp.concatenate(
                        [
                            source[pl.ds(pl.multiple_of((((h * chunks + c) * blocks + d) * STEP + p) * TILE, TILE), TILE), :]
                            for h in range(cuts)
                            for d in range(blocks)
                        ],
                        axis=0,
                    )
                    for source in (modes, others)
                ],
                axis=1,
            )
            high, low = split(both)
            result = dot(table_w[...], jnp.concatenate([high, high, low], axis=0))
            line[slot, 0, p] = result[:, :LANES]
            line[slot, 1, p] = result[:, LANES:]

        for s in range(2):
            keep(c, s).start()

    for copy in tables[:2]:
        copy.wait()

    @pl.loop(0, bites)
    def _(b):
        density(b)

        @pl.when(b == 0)
        def _():
            pl.semaphore_wait(barrier, blocks)

        @pl.when(lax.rem(b, per) == per - 1)
        def _():
            send_x(b // per).start()

        @pl.when((b >= LEAD) & (lax.rem(b - LEAD, PACE) == 0))
        def _():
            spectrum((b - LEAD) // PACE)

    first = (bites - 1 - LEAD) // PACE + 1

    @pl.loop(chunks, items)
    def _(e):
        send_x(e).start()

    prepare()

    last = cuts - 1
    base = last * chunks + ratio + LATER - 1

    @pl.loop(first, items)
    def _(e):
        spectrum(e)
        at = chunks + LATE - groups

        @pl.when((e >= at) & (e < at + groups - 1))
        def _():
            gather(0, e - at)

        @pl.when(e == at + groups - 1)
        def _():
            gather_last(0)

        @pl.when((e >= at + groups) & (e < at + 2 * groups))
        def _():
            filtered(0, e - at - groups)

        @pl.when((e >= base) & (lax.rem(e - base + ratio * items, ratio) == 0))
        def _():
            gather(last, (e - base) // ratio)

        k = e - (items - EARLY)

        @pl.when(k >= 1)
        def _():
            hand_over(k - 1)

        @pl.when(k >= 0)
        def _():
            give_back(k)

    for e in range(EARLY, EARLY + WINDOW - 1):
        give_back(e)

    done = (items - 1 - base) // ratio + 1

    @pl.loop(EARLY - 1, items)
    def _(e):
        ahead = e + WINDOW
        hand_over(e)

        @pl.when(ahead < items)
        def _():
            give_back(ahead)

        @pl.when((e >= REST) & (e - REST + done < groups - 1))
        def _():
            gather(last, e - REST + done)

        @pl.when(e == MIDDLE)
        def _():
            gather_last(last)

        after = ahead + 1 - last * chunks

        @pl.when((after >= 0) & (after < chunks) & (lax.rem(after + items * ratio, ratio) == 0))
        def _():
            filtered(last, after // ratio)

        @pl.when(e > last * chunks)
        def _():
            inverse(e - last * chunks - 1)

    inverse(chunks - 1)

    for c in (chunks - 2, chunks - 1):
        for s in range(2):
            keep(c, s).wait()

    @pl.loop(0, items)
    def _(e):
        send_x(e).wait_send()
        arrivals(f_send.at[e]).wait()
        arrivals(b_send.at[e]).wait()
        send_h(e).wait_send()


def last_kernel(lines, inverse_y, potential, given, made, table, in_sem, out_sem, table_sem):
    planes, nx, ny = potential.shape

    def take(i):
        return pltpu.make_async_copy(lines.at[:, pl.ds(i * PART, PART)], given.at[i], in_sem.at[i])

    def put(i):
        return pltpu.make_async_copy(made.at[i], potential.at[pl.ds(i * PART, PART)], out_sem.at[i])

    whole = pltpu.make_async_copy(inverse_y, table, table_sem)
    whole.start()

    @pl.loop(0, planes // PART)
    def _(i):
        take(i).start()

    whole.wait()

    @pl.loop(0, planes // PART)
    def _(i):
        take(i).wait()
        both = [given[i, s].reshape(PART * nx, LANES) for s in range(2)]
        high, low = split(jnp.concatenate(both, axis=1))
        made[i] = dot(jnp.concatenate([high, low, high], axis=1), table[...]).reshape(PART, nx, ny)
        put(i).start()

    @pl.loop(0, planes // PART)
    def _(i):
        put(i).wait()


def fused(orbitals, kweights, occupations, z_basis, z_eigen):
    points, bands, parts, planes, nx, ny = orbitals.shape
    nz = z_basis.shape[0]
    blocks = lax.axis_size("grid")
    chunks = planes // STEP
    groups = planes // TILE
    cuts = nx // (blocks * TILE)
    items = cuts * chunks
    depth = blocks * TILE
    pairs = TILE // 2
    order = np.arange(nx).reshape(blocks, cuts, TILE).transpose(1, 0, 2).reshape(nx)
    table_x, scaled_x = basis_tables(nx)
    table_y, scaled_y = basis_tables(ny)
    high, low = halves(table_y)
    stack = np.concatenate([high.T, high.T, low.T], axis=0)
    forward_y = np.stack([np.roll(stack, LANES, axis=1), stack])
    high, low = halves(table_x[order])
    forward_x = np.concatenate([high, low, high], axis=1)
    high, low = halves(scaled_x[order].T)
    inverse_x = np.concatenate([high, low, high], axis=1)
    high, low = halves(scaled_y)
    inverse_y = np.concatenate([high, high, low], axis=0)
    wave_y = ((2.0 * np.sin(np.pi * np.arange(ny) / ny)) ** 2).astype(np.float32).reshape(2, LANES)
    wave_x = ((2.0 * np.sin(np.pi * np.arange(nx) / nx)) ** 2).astype(np.float32)

    anywhere = pl.BlockSpec(memory_space=pl.ANY)
    scalars = pl.BlockSpec(memory_space=pltpu.SMEM)
    vector = pl.BlockSpec(memory_space=pltpu.VMEM)
    dma = pltpu.SemaphoreType.DMA
    exchanged = pl.pallas_call(
        fused_kernel,
        out_shape=jax.ShapeDtypeStruct((2, planes, nx, LANES), f32),
        in_specs=[anywhere, scalars, scalars, anywhere, anywhere, anywhere, anywhere, anywhere, vector, scalars],
        out_specs=anywhere,
        scratch_shapes=[
            pltpu.VMEM((SLOTS, points, bands, parts, BITE, nx, ny), bf16),
            pltpu.VMEM((BITE * nx, 2 * ny), bf16),
            pltpu.VMEM((3 * ny, 2 * LANES), bf16),
            pltpu.VMEM((nx, 3 * nx), bf16),
            pltpu.VMEM((nx, 3 * nx), bf16),
            pltpu.VMEM((blocks, planes, nz), f32),
            pltpu.VMEM((1, nz), f32),
            pltpu.VMEM((planes * nx, LANES), f32),
            pltpu.VMEM((planes * nx, LANES), f32),
            pltpu.VMEM((planes * nx, LANES), f32),
            pltpu.VMEM((planes * nx, LANES), f32),
            pltpu.VMEM((pairs, nz, 2 * LANES), f32),
            pltpu.VMEM((pairs, nz, 2 * LANES), bf16),
            pltpu.VMEM((pairs, nz, 2 * LANES), bf16),
            pltpu.VMEM((groups, depth, nz), bf16),
            pltpu.VMEM((groups, depth, nz), bf16),
            pltpu.VMEM((groups, nz, 3 * depth), bf16),
            pltpu.VMEM((nz, LANES), f32),
            pltpu.VMEM((planes * nx, LANES), f32),
            pltpu.VMEM((planes * nx, LANES), f32),
            pltpu.VMEM((2, 2, STEP, nx, LANES), f32),
            dma((SLOTS,)),
            dma((5,)),
        ]
        + [dma((items,))] * 8
        + [dma((2, 2))],
        compiler_params=pltpu.CompilerParams(
            collective_id=0, has_side_effects=True, vmem_limit_bytes=62 * 1024 * 1024
        ),
        name="exchange",
    )(
        orbitals, kweights, occupations, z_basis.reshape(blocks, planes, nz), z_eigen.reshape(1, nz),
        jnp.asarray(forward_y), jnp.asarray(forward_x), jnp.asarray(inverse_x),
        jnp.asarray(wave_y), jnp.asarray(wave_x),
    )
    counted = planes // PART
    return pl.pallas_call(
        last_kernel,
        out_shape=jax.ShapeDtypeStruct((planes, nx, ny), f32),
        in_specs=[anywhere, anywhere],
        out_specs=anywhere,
        scratch_shapes=[
            pltpu.VMEM((counted, 2, PART, nx, LANES), f32),
            pltpu.VMEM((counted, PART, nx, ny), f32),
            pltpu.VMEM((3 * ny, ny), bf16),
            dma((counted,)),
            dma((counted,)),
            dma,
        ],
        compiler_params=pltpu.CompilerParams(vmem_limit_bytes=62 * 1024 * 1024),
        name="last",
    )(exchanged, jnp.asarray(inverse_y))


def real_basis(length):
    position = jnp.arange(length, dtype=jnp.int32)
    product = position[:, None] * position[None, :] % length
    angles = product.astype(jnp.float32) * (2.0 * jnp.pi / length)
    lower = position[:, None] <= length // 2
    table = jnp.where(lower, jnp.cos(angles), jnp.sin(angles))
    edges = (position == 0) | (position == length // 2)
    weights = jnp.where(edges, 1.0, 2.0).astype(jnp.float32) / length
    return (table, table * weights[:, None])


def on_device(orbitals, kweights, occupations, z_basis, z_eigen):
    points, band_count, _, planes, x_length, y_length = orbitals.shape
    z_length = z_basis.shape[0]
    groups = lax.axis_size("kpt")
    blocks = lax.axis_size("grid")
    group = lax.axis_index("kpt")
    ky_count = y_length // groups
    kx_count = x_length // blocks
    step = max(planes // CHUNKS, 1)
    chunks = planes // step
    factor = (kweights[:, None] * occupations).astype(jnp.float32) / (16.0 * points * band_count)
    table_x, scaled_x = real_basis(x_length)
    table_y, scaled_y = real_basis(y_length)

    def part_of(table, shift):
        start = lax.rem(group + shift, groups) * ky_count
        return lax.dynamic_slice_in_dim(table, start, ky_count, 0)

    def shifted_by(shift):
        return [(g, (g + shift) % groups) for g in range(groups)]

    forward_y = [part_of(table_y, shift) for shift in range(groups)]
    inverse_y = [part_of(scaled_y, shift) for shift in range(groups)]
    basis = z_basis.reshape(blocks, planes, z_length)

    projected = None
    for chunk in range(chunks):
        rows = slice(chunk * step, (chunk + 1) * step)
        values = orbitals[:, :, :, rows].astype(jnp.float32)
        density = jnp.sum(factor[:, :, None, None, None, None] * values * values, axis=(0, 1, 2))
        along = jnp.einsum("zxy,ky->zxk", density, forward_y[0], precision=precise)
        for shift in range(1, groups):
            other = jnp.einsum("zxy,ky->zxk", density, forward_y[shift], precision=precise)
            arrived = lax.ppermute(other, "kpt", shifted_by(shift))
            along = along + arrived
        spectrum = jnp.einsum("jx,zxk->zjk", table_x, along, precision=precise)
        column = lax.all_to_all(
            spectrum.reshape(step, blocks, kx_count, ky_count), "grid", split_axis=1, concat_axis=0, tiled=True
        ).reshape(blocks * step, kx_count, ky_count)
        z_rows = basis[:, rows].reshape(blocks * step, z_length)
        term = jnp.einsum("zj,zab->jab", z_rows, column, precision=precise)
        projected = term if projected is None else projected + term

    wave_x = (lax.axis_index("grid") * kx_count + jnp.arange(kx_count, dtype=jnp.int32)).astype(jnp.float32)
    wave_y = (group * ky_count + jnp.arange(ky_count, dtype=jnp.int32)).astype(jnp.float32)
    shift_x = 2.0 * jnp.sin(jnp.pi * wave_x / x_length)
    shift_y = 2.0 * jnp.sin(jnp.pi * wave_y / y_length)
    shifted = shift_x[:, None] ** 2 + shift_y[None, :] ** 2
    scaled = projected * (1.0 / (z_eigen[:, None, None] + shifted[None]))

    outputs = []
    for chunk in range(chunks):
        rows = slice(chunk * step, (chunk + 1) * step)
        z_rows = basis[:, rows].reshape(blocks * step, z_length)
        filtered = jnp.einsum("zj,jab->zab", z_rows, scaled, precision=precise)
        modes = lax.all_to_all(
            filtered.reshape(blocks, step, kx_count, ky_count), "grid", split_axis=0, concat_axis=0, tiled=True
        )
        half = jnp.einsum(
            "jx,zjk->zxk",
            scaled_x,
            modes.transpose(1, 0, 2, 3).reshape(step, x_length, ky_count),
            precision=precise,
        )
        total = jnp.einsum("zxk,ky->zxy", half, inverse_y[0], precision=precise)
        for shift in range(1, groups):
            arrived = lax.ppermute(half, "kpt", shifted_by(groups - shift))
            total = total + jnp.einsum("zxk,ky->zxy", arrived, inverse_y[shift], precision=precise)
        outputs.append(total)
    return jnp.concatenate(outputs, axis=0)


def solution(mesh):
    groups, blocks = mesh.shape["kpt"], mesh.shape["grid"]
    specs = dict(
        mesh=mesh,
        in_specs=(P("kpt", None, None, "grid", None, None), P("kpt"), P("kpt", None), P(), P()),
        out_specs=P("grid", None, None),
        check_vma=False,
    )
    plain = jax.shard_map(on_device, **specs)
    kernels = jax.shard_map(fused, **specs)

    def step(orbitals, *rest):
        _, _, _, nz, nx, ny = orbitals.shape
        fits = groups == 2 and ny == 2 * LANES and nx == 2 * TILE * blocks and nz % (TILE * blocks) == 0
        return (kernels if fits else plain)(orbitals, *rest)

    return step
```
